256 devices in a mesh: pole: 8 (over x, core), row: 4 (over z_lo), col: 8 (over z_hi, y).
Axes of the slice: x: 4, y: 4, z: 8 (z_hi: 2, z_lo: 4; z = z_hi * 4 + z_lo), core: 2. Of those that a mesh axis runs over, the one named last changes fastest.
Arguments:
- anc_inverse: bfloat16 [8, 2, 4, 768, 3072], P('pole', None, None, 'col', 'row'), may hold values from -6 to 6
- panel: bfloat16 [8, 2, 3072, 4096], P('pole', None, ('row', 'col')), may hold values from -0.109375 to 0.109375
- pattern: int32 [32, 8], replicated, may hold values 0 or 1
- diag_inverse: bfloat16 [8, 2, 4096, 512], P('pole', None, 'col', 'row'), may hold values from -6 to 6
- pole_weights: float32 [8, 2], P('pole'), may hold values from -4 to 4
Outputs:
- inv_panel: float32 [8, 2, 3072, 4096], P('pole', None, 'row', 'col')
- inv_diag: bfloat16 [8, 2, 4096, 512], P('pole', None, 'col', 'row')
- density: float32 [4096, 512], P('col', 'row')
The draws below stay inside these ranges and needn't reach their ends.
All inputs are finite; a program needn't handle non-finite values.
Results may differ from the reference program's by a relative error of at most 0.013.
Values may be sent and summed in bfloat16 or wider, within the bound.
A program may use at most 128 MiB of HBM per device.

```python
import jax
import jax.numpy as jnp
from jax import lax

W = 512
ANC_DEV = 96
POLES = 8
NK = 8
KW = 4096
NFB = 32
NA = 3072
NQ = 4


def plant(values, rng, smallest, high):
    place = [jax.random.randint(jax.random.fold_in(rng, axis), (), 0, length) for axis, length in enumerate(values.shape)]
    main_axis = values.shape.index(max(values.shape))
    next_to = place[:main_axis] + [(place[main_axis] + 1) % values.shape[main_axis]] + place[main_axis + 1:]
    return values.at[tuple(place)].set(smallest).at[tuple(next_to)].set(high)


def block_scale(key, dims, pieces, smallest, top_value):
    factor_of = 1.0
    for axis_at, blocks in pieces:
        steps = jax.random.uniform(jax.random.fold_in(jax.random.fold_in(key, 6), axis_at), (blocks,), jnp.float32, smallest / len(pieces), top_value / len(pieces))
        factor_of = factor_of * jnp.repeat(jnp.exp(steps), dims[axis_at] // blocks).reshape((-1,) + (1,) * (len(dims) - 1 - axis_at))
    return factor_of


def bell_draw(own_key, dims, spread, most, split=(), held_as=jnp.bfloat16):
    loudness = block_scale(own_key, dims, split, -0.22, 0.18) if split else 1.0
    values = jax.random.normal(own_key, dims, jnp.float32) * spread * loudness
    return jnp.minimum(jnp.maximum(values, -most), most).astype(held_as)


def setup_inputs(seed: int = 0) -> dict:
    splits = jax.random.split(jax.random.key(seed), 6)
    return {
        "anc_inverse": bell_draw(splits[0], (POLES, 2, NQ, NA // NQ, NA), 1.0, 6.0, ((0, 8), (3, 8), (4, 4))),
        "panel": bell_draw(splits[1], (POLES, 2, NA, KW), NA ** -0.5, 0.109375, ((0, 8), (2, 32))),
        "pattern": plant((jax.random.randint(splits[2], (NFB, NK), 0, 3) < 2).astype(jnp.int32), jax.random.fold_in(splits[2], 1), 0, 1),
        "diag_inverse": bell_draw(splits[3], (POLES, 2, KW, W), 1.0, 6.0, ((0, 8), (2, 8), (3, 4))),
        "pole_weights": bell_draw(splits[4], (POLES, 2), 1.0, 4.0, ((0, 8),), jnp.float32),
    }


def complex_product(left_re, left_im, right_re, right_im):
    exact = lax.Precision.HIGHEST
    left_re = left_re.astype(jnp.float32)
    left_im = left_im.astype(jnp.float32)
    right_re = right_re.astype(jnp.float32)
    right_im = right_im.astype(jnp.float32)
    real_part = jnp.dot(left_re.T, right_re, precision=exact) - jnp.dot(left_im.T, right_im, precision=exact)
    imag_part = jnp.dot(left_im.T, right_re, precision=exact) + jnp.dot(left_re.T, right_im, precision=exact)
    return real_part, imag_part


def reference(anc_inverse, panel, pattern, diag_inverse, pole_weights):
    exact = lax.Precision.HIGHEST
    keep_mask = jnp.repeat(jnp.repeat(pattern.astype(jnp.bfloat16), W, axis=1), ANC_DEV, axis=0)

    def contract(first, second):
        return jnp.einsum('jka,jkb->kab', first, second, precision=exact)

    def one_pole(inputs):
        ancestor, factor, diagonal = inputs
        transposed = ancestor.reshape(2, NA, NA)
        masked = factor * keep_mask[None]
        prod_re, prod_im = complex_product(transposed[0], transposed[1], masked[0], masked[1])
        result_panel = jnp.stack([-prod_re, -prod_im])
        rounded = lax.optimization_barrier(result_panel.astype(jnp.bfloat16)).astype(jnp.float32)
        factor_full = masked.astype(jnp.float32).reshape(2, NA, NK, W)
        panel_full = rounded.reshape(2, NA, NK, W)
        diag_re = contract(factor_full[0], panel_full[0]) - contract(factor_full[1], panel_full[1])
        diag_im = contract(factor_full[0], panel_full[1]) + contract(factor_full[1], panel_full[0])
        result_diag = diagonal.astype(jnp.float32) - jnp.stack([diag_re, diag_im]).reshape(2, KW, W)
        return result_panel, result_diag

    inv_panel, diag_full = lax.map(one_pole, (anc_inverse, panel, diag_inverse))
    density = jnp.einsum('p,pab->ab', pole_weights[:, 0], diag_full[:, 1], precision=exact)
    density = density + jnp.einsum('p,pab->ab', pole_weights[:, 1], diag_full[:, 0], precision=exact)
    return inv_panel, diag_full.astype(jnp.bfloat16), density
```

```python
import jax
import jax.numpy as jnp
from jax import lax
from jax.experimental import pallas as pl
from jax.experimental.pallas import tpu as pltpu
from jax.sharding import PartitionSpec as P

MESH = pl.DeviceIdType.MESH
F32 = jnp.float32
BF16 = jnp.bfloat16

E = 96
ROWS = 768
LN = 128
ORDER = (0, 3, 1, 2)


def copy_to(src, dst, send_sem, recv_sem, dev):
    return pltpu.make_async_remote_copy(
        src_ref=src,
        dst_ref=dst,
        send_sem=send_sem,
        recv_sem=recv_sem,
        device_id=dev,
        device_id_type=MESH,
    )


def dot(a, b, dims=(1, 0)):
    return lax.dot_general(
        a, b, (((dims[0],), (dims[1],)), ((), ())), preferred_element_type=F32
    )


def kernel(
    pat, wgt, g_in, p_in, d_in,
    x_out, id_out, den_out,
    gbuf, gt, lsrc, lbuf, loth, lrel, acc, xs, xb, dsend, drecv, term, tpair, px, dh, dp,
    a_s, a_r, gz_s, gz_r, gy_s, gy_r, gr_s, gr_r, gc_s, gc_r,
    lp_s, lp_r, lm_s, lm_r, x_s, x_r, d_s, d_r, t_s, t_r, p_s, p_r, h_s, h_r, o_s,
):
    pole = lax.axis_index("pole")
    r = lax.axis_index("row")
    c = lax.axis_index("col")
    h = c // 4
    y = lax.rem(c, 4)
    z = 4 * h + r
    oth = 1 - h
    core = lax.rem(pole, 2)
    xx = pole // 2

    def at_y(d):
        return {"col": 4 * h + lax.rem(y + d, 4)}

    def at_z(d):
        zz = lax.rem(z + d, 8)
        return {"row": lax.rem(zz, 4), "col": (zz // 4) * 4 + y}

    def at_row(d):
        return {"row": lax.rem(r + d, 4)}

    def at_x(d):
        return {"pole": lax.rem(xx + d, 4) * 2 + core}

    partner = {"pole": 2 * xx + 1 - core}
    across = {"col": 4 * oth + y}

    bar = pltpu.get_barrier_semaphore()
    peers = [at_y(1), at_y(2), at_y(3), at_z(1), at_z(7), across, partner]
    peers += [at_row(d) for d in (1, 2, 3)] + [at_x(d) for d in (1, 2, 3)]
    for dev in peers:
        pl.semaphore_signal(bar, inc=1, device_id=dev, device_id_type=MESH)
    pl.semaphore_wait(bar, len(peers))

    def gz(t):
        return copy_to(g_in.at[0, t], gbuf.at[h, t, :, y], gz_s.at[t], gz_r.at[t], across)

    for t in (0, 1):
        gz(t).start()

    fine = r * 8 + c
    for k in range(8):
        keep = pat[fine, k].astype(F32)
        for j in range(4):
            lo = k * 512 + ORDER[j] * LN
            for t in (0, 1):
                blk = p_in[0, t, :, lo:lo + LN].astype(F32) * keep
                lsrc[k, j, :, t * LN:(t + 1) * LN] = blk.astype(BF16)
    gbuf[h, :, :, y] = g_in[0]

    def to_col(d, which):
        k = (h if which == 0 else oth) * 4 + lax.rem(y + d, 4)
        dst = lbuf.at[:, z, y] if which == 0 else loth.at[:, y]
        return copy_to(lsrc.at[k], dst, a_s.at[d - 1, which], a_r.at[d - 1, which], at_y(d))

    for which in (1, 0):
        for d in (1, 3, 2):
            to_col(d, which).start()

    def gy(way, t):
        return copy_to(
            g_in.at[0, t], gbuf.at[h, t, :, y], gy_s.at[way, t], gy_r.at[way, t], at_y(1 if way == 0 else 3)
        )

    for i in (0, 1):
        gy(0, i).start()
        gy(1, 1 - i).start()

    lbuf[:, z, y] = lsrc[h * 4 + y]
    loth[:, y] = lsrc[oth * 4 + y]

    for which in (1, 0):
        for d in (1, 3, 2):
            to_col(d, which).wait_recv()

    def up(j, i, src, zp):
        return copy_to(src, lbuf.at[j, zp], lp_s.at[j, i], lp_r.at[j, i], at_z(1))

    def down(j, i, src, zp):
        return copy_to(src, lbuf.at[j, zp], lm_s.at[j, i], lm_r.at[j, i], at_z(7))

    def extra(j, d):
        return copy_to(loth.at[j], lrel.at[j], x_s.at[j], x_r.at[j], at_z(d))

    @pl.loop(0, 4)
    def _(j):
        @pl.when(r == 2)
        def _():
            extra(j, 1).start()

        @pl.when(r == 1)
        def _():
            extra(j, 7).start()

        @pl.when(r == 3)
        def _():
            up(j, 1, loth.at[j], z).start()

        @pl.when(r == 0)
        def _():
            down(j, 1, loth.at[j], z).start()

    @pl.loop(0, 4)
    def _(j):
        @pl.when(r < 3)
        def _():
            up(j, r + 2, lbuf.at[j, z], z).start()

        @pl.when(r > 0)
        def _():
            down(j, 5 - r, lbuf.at[j, z], z).start()

    def relay(way):
        t = way
        frm = lax.rem(y + (3 if way == 0 else 1), 4)
        ref = gbuf.at[h, t, :, frm]
        return copy_to(ref, ref, gr_s.at[way], gr_r.at[way], at_y(1 if way == 0 else 3))

    gy(0, 0).wait_recv()
    relay(0).start()
    gy(1, 1).wait_recv()
    relay(1).start()

    def gc(d, t):
        ref = gbuf.at[oth, t, :, y]
        return copy_to(ref, ref, gc_s.at[d - 1, t], gc_r.at[d - 1, t], at_y(d))

    for t in (0, 1):
        gz(t).wait_recv()
        for d in (1, 3, 2):
            gc(d, t).start()

    @pl.loop(0, 4)
    def _(j):
        @pl.when(r == 3)
        def _():
            extra(j, 1).wait_recv()
            up(j, 0, lrel.at[j], 4 * h + 2).start()

        @pl.when(r == 0)
        def _():
            extra(j, 7).wait_recv()
            down(j, 0, lrel.at[j], 4 * h + 1).start()

    gy(0, 1).wait_recv()
    gy(1, 0).wait_recv()
    relay(0).wait_recv()
    relay(1).wait_recv()

    def turn(half):
        @pl.loop(0, 4)
        def _(q):
            for t in (0, 1):
                gt[half * 4 + q, t] = gbuf[half, t, q].reshape(4 * E, ROWS).T

    turn(h)

    def compute(slot, j, zp):
        right = lbuf[j, zp].reshape(4 * E, 2 * LN)
        for t in (0, 1):
            acc[slot, t] += dot(gt[zp, t], right)

    def first(slot, j):
        right = lbuf[j, z].reshape(4 * E, 2 * LN)
        for t in (0, 1):
            acc[slot, t] = dot(gt[z, t], right)

    def stream(j, work):
        for slot, jj in work:
            first(slot, jj)

        @pl.loop(0, 5)
        def _(i):
            zp = lax.rem(4 * h + 6 + i, 8)
            zm = lax.rem(4 * h + 5 - i + 8, 8)

            @pl.when(i < r + 2)
            def _():
                one = up(j, i, lbuf.at[j, zp], zp)
                one.wait_recv()

                @pl.when(r < 3)
                def _():
                    one.start()

            @pl.when(i < 5 - r)
            def _():
                one = down(j, i, lbuf.at[j, zm], zm)
                one.wait_recv()

                @pl.when(r > 0)
                def _():
                    one.start()

            @pl.when(i < r + 2)
            def _():
                for slot, jj in work:
                    compute(slot, jj, zp)

            @pl.when(i < 5 - r)
            def _():
                for slot, jj in work:
                    compute(slot, jj, zm)

    def out_copy(j):
        cols = pl.ds(ORDER[j] * LN, LN)
        return pltpu.make_async_copy(xs.at[:, :, cols], x_out.at[0, :, :, cols], o_s.at[j])

    def finish(slot, j):
        lo = ORDER[j] * LN

        @pl.loop(0, 8)
        def _(b):
            rows = pl.ds(b * E, E)
            re = acc[slot, 1, rows, LN:] - acc[slot, 0, rows, :LN]
            im = -(acc[slot, 0, rows, LN:] + acc[slot, 1, rows, :LN])
            xs[0, rows, lo:lo + LN] = re
            xs[1, rows, lo:lo + LN] = im
            xb[j, rows, :LN] = re.astype(BF16)
            xb[j, rows, LN:] = im.astype(BF16)

        out_copy(j).start()

    def diag(ja, jb):
        low = lbuf[ja, r].reshape(4 * E, 2 * LN)
        high = lbuf[ja, 4 + r].reshape(4 * E, 2 * LN)
        both = dot(low, xb[jb, :4 * E], (0, 0)) + dot(high, xb[jb, 4 * E:], (0, 0))
        lo = ORDER[ja] * LN
        dsend[ORDER[jb], 0, lo:lo + LN] = (both[:LN, :LN] - both[LN:, LN:]).astype(BF16)
        dsend[ORDER[jb], 1, lo:lo + LN] = (both[:LN, LN:] + both[LN:, :LN]).astype(BF16)

    stream(0, ())
    for t in (0, 1):
        for d in (1, 3, 2):
            gc(d, t).wait_recv()
    turn(oth)
    stream(1, ((0, 0),))
    finish(0, 0)
    stream(2, ((1, 1),))
    finish(1, 1)
    stream(3, ((0, 2), (1, 3)))
    finish(0, 2)
    finish(1, 3)

    for jb in range(4):
        for ja in range(4):
            diag(ja, jb)

    def share(d):
        return copy_to(
            dsend.at[lax.rem(r + d, 4)], drecv.at[d - 1], d_s.at[d - 1], d_r.at[d - 1], at_row(d)
        )

    for d in (1, 2, 3):
        share(d).start()
    for d in (1, 2, 3):
        share(d).wait_recv()

    def full(t):
        got = dsend[r, t].astype(F32)
        for d in range(3):
            got += drecv[d, t].astype(F32)
        return d_in[0, t].astype(F32) - got

    re = full(0)
    im = full(1)
    id_out[0, 0] = re.astype(BF16)
    id_out[0, 1] = im.astype(BF16)
    term[...] = wgt[0, 0] * im + wgt[0, 1] * re

    mine = pl.ds(pl.multiple_of(core * 256, 256), 256)
    other = pl.ds(pl.multiple_of((1 - core) * 256, 256), 256)
    pair = copy_to(term.at[other], tpair, t_s, t_r, partner)
    pair.start()
    pair.wait_recv()
    px[xx] = (term[mine, :] + tpair[...]).astype(BF16)

    def along(d):
        return copy_to(px.at[xx], px.at[xx], p_s.at[d - 1], p_r.at[d - 1], at_x(d))

    for d in (1, 3, 2):
        along(d).start()
    for d in (1, 3, 2):
        along(d).wait_recv()
    half = px[0].astype(F32)
    for k in range(1, 4):
        half += px[k].astype(F32)
    dh[...] = half
    den_out[mine, :] = half
    swap = copy_to(dh, dp, h_s, h_r, partner)
    swap.start()
    swap.wait_recv()
    den_out[other, :] = dp[...]

    for t in (0, 1):
        gz(t).wait_send()
        gy(0, t).wait_send()
        gy(1, t).wait_send()
        relay(t).wait_send()
        for d in (1, 2, 3):
            gc(d, t).wait_send()
            to_col(d, t).wait_send()
    for d in (1, 2, 3):
        share(d).wait_send()
        along(d).wait_send()
    pair.wait_send()
    swap.wait_send()

    @pl.loop(0, 4)
    def _(j):
        @pl.when((r == 1) | (r == 2))
        def _():
            extra(j, 1).wait_send()

        @pl.loop(0, 5)
        def _(i):
            @pl.when(((r < 3) & (i < r + 3)) | ((r == 3) & (i < 2)))
            def _():
                up(j, i, lbuf.at[j, z], z).wait_send()

            @pl.when(((r > 0) & (i < 6 - r)) | ((r == 0) & (i < 2)))
            def _():
                down(j, i, lbuf.at[j, z], z).wait_send()

    for j in range(4):
        out_copy(j).wait()


def body(anc_inverse, panel, pattern, diag_inverse, pole_weights):
    vmem = pl.BlockSpec(memory_space=pltpu.VMEM)
    smem = pl.BlockSpec(memory_space=pltpu.SMEM)
    dma = pltpu.SemaphoreType.DMA
    sems = [(3, 2), (2,), (2, 2), (2,), (3, 2), (4, 5), (4, 5), (4,), (3,), None, (3,), None]
    pairs = []
    for shape in sems:
        one = dma if shape is None else dma(shape)
        pairs += [one, one]
    return pl.pallas_call(
        kernel,
        out_shape=(
            jax.ShapeDtypeStruct((1, 2, ROWS, 512), F32),
            jax.ShapeDtypeStruct((1, 2, 512, LN), BF16),
            jax.ShapeDtypeStruct((512, LN), F32),
        ),
        in_specs=[smem, smem, vmem, vmem, vmem],
        out_specs=(pl.BlockSpec(memory_space=pl.ANY), vmem, vmem),
        scratch_shapes=[
            pltpu.VMEM((2, 2, 4, 4, E, ROWS), BF16),
            pltpu.VMEM((8, 2, ROWS, 4 * E), BF16),
            pltpu.VMEM((8, 4, E, 2 * LN), BF16),
            pltpu.VMEM((4, 8, 4, E, 2 * LN), BF16),
            pltpu.VMEM((4, 4, E, 2 * LN), BF16),
            pltpu.VMEM((4, 4, E, 2 * LN), BF16),
            pltpu.VMEM((2, 2, ROWS, 2 * LN), F32),
            pltpu.VMEM((2, ROWS, 512), F32),
            pltpu.VMEM((4, ROWS, 2 * LN), BF16),
            pltpu.VMEM((4, 2, 512, LN), BF16),
            pltpu.VMEM((3, 2, 512, LN), BF16),
            pltpu.VMEM((512, LN), F32),
            pltpu.VMEM((256, LN), F32),
            pltpu.VMEM((4, 256, LN), BF16),
            pltpu.VMEM((256, LN), F32),
            pltpu.VMEM((256, LN), F32),
            *pairs,
            dma((4,)),
        ],
        compiler_params=pltpu.CompilerParams(
            collective_id=0, has_side_effects=True, vmem_limit_bytes=60 * 1024 * 1024
        ),
    )(pattern, pole_weights, anc_inverse, panel, diag_inverse)


def solution(mesh):
    placed = (
        P("pole", None, None, "col", "row"),
        P("pole", None, ("row", "col"), None),
        P(),
        P("pole", None, "col", "row"),
        P("pole", None),
    )
    return jax.shard_map(
        body,
        mesh=mesh,
        in_specs=placed,
        out_specs=(P("pole", None, "row", "col"), P("pole", None, "col", "row"), P("col", "row")),
        check_vma=False,
    )
```

```python
import jax
import jax.numpy as jnp
from jax import lax
from jax.experimental import pallas as pl
from jax.experimental.pallas import tpu as pltpu
from jax.sharding import PartitionSpec as P

MESH = pl.DeviceIdType.MESH
F32 = jnp.float32
BF16 = jnp.bfloat16

E = 96
ROWS = 768
LN = 128
ORDER = (0, 3, 1, 2)


def copy_to(src, dst, send_sem, recv_sem, dev):
    return pltpu.make_async_remote_copy(
        src_ref=src,
        dst_ref=dst,
        send_sem=send_sem,
        recv_sem=recv_sem,
        device_id=dev,
        device_id_type=MESH,
    )


def dot(a, b, dims=(1, 0)):
    return lax.dot_general(
        a, b, (((dims[0],), (dims[1],)), ((), ())), preferred_element_type=F32
    )


def kernel(
    pat, wgt, g_in, p_in, d_in,
    x_out, id_out, den_out,
    gbuf, gt, lsrc, lbuf, loth, lrel, acc, xs, xb, dsend, drecv, term, tpair, px, dh, dp,
    a_s, a_r, gz_s, gz_r, gy_s, gy_r, gr_s, gr_r, gc_s, gc_r,
    lp_s, lp_r, lm_s, lm_r, x_s, x_r, d_s, d_r, t_s, t_r, p_s, p_r, h_s, h_r, o_s,
):
    pole = lax.axis_index("pole")
    r = lax.axis_index("row")
    c = lax.axis_index("col")
    h = c // 4
    y = lax.rem(c, 4)
    z = 4 * h + r
    oth = 1 - h
    core = lax.rem(pole, 2)
    xx = pole // 2

    def at_y(d):
        return {"col": 4 * h + lax.rem(y + d, 4)}

    def at_z(d):
        zz = lax.rem(z + d, 8)
        return {"row": lax.rem(zz, 4), "col": (zz // 4) * 4 + y}

    def at_row(d):
        return {"row": lax.rem(r + d, 4)}

    def at_x(d):
        return {"pole": lax.rem(xx + d, 4) * 2 + core}

    partner = {"pole": 2 * xx + 1 - core}
    across = {"col": 4 * oth + y}

    bar = pltpu.get_barrier_semaphore()
    peers = [at_y(1), at_y(2), at_y(3), at_z(1), at_z(7), across, partner]
    peers += [at_row(d) for d in (1, 2, 3)] + [at_x(d) for d in (1, 2, 3)]
    for dev in peers:
        pl.semaphore_signal(bar, inc=1, device_id=dev, device_id_type=MESH)
    pl.semaphore_wait(bar, len(peers))

    def gz(t):
        return copy_to(g_in.at[0, t], gbuf.at[h, t, :, y], gz_s.at[t], gz_r.at[t], across)

    for t in (0, 1):
        gz(t).start()

    fine = r * 8 + c
    for k in range(8):
        keep = pat[k, fine].astype(F32)
        for j in range(4):
            lo = k * 512 + ORDER[j] * LN
            for t in (0, 1):
                blk = p_in[0, t, :, lo:lo + LN].astype(F32) * keep
                lsrc[k, j, :, t * LN:(t + 1) * LN] = blk.astype(BF16)
    gbuf[h, :, :, y] = g_in[0]

    def to_col(d, which):
        k = (h if which == 0 else oth) * 4 + lax.rem(y + d, 4)
        dst = lbuf.at[:, z, y] if which == 0 else loth.at[:, y]
        return copy_to(lsrc.at[k], dst, a_s.at[d - 1, which], a_r.at[d - 1, which], at_y(d))

    for which in (1, 0):
        for d in (1, 3, 2):
            to_col(d, which).start()

    def gy(way, t):
        return copy_to(
            g_in.at[0, t], gbuf.at[h, t, :, y], gy_s.at[way, t], gy_r.at[way, t], at_y(1 if way == 0 else 3)
        )

    for i in (0, 1):
        gy(0, i).start()
        gy(1, 1 - i).start()

    lbuf[:, z, y] = lsrc[h * 4 + y]
    loth[:, y] = lsrc[oth * 4 + y]

    for which in (1, 0):
        for d in (1, 3, 2):
            to_col(d, which).wait_recv()

    def up(j, i, src, zp):
        return copy_to(src, lbuf.at[j, zp], lp_s.at[j, i], lp_r.at[j, i], at_z(1))

    def down(j, i, src, zp):
        return copy_to(src, lbuf.at[j, zp], lm_s.at[j, i], lm_r.at[j, i], at_z(7))

    def extra(j, d):
        return copy_to(loth.at[j], lrel.at[j], x_s.at[j], x_r.at[j], at_z(d))

    def launch(j):
        @pl.when(r == 2)
        def _():
            extra(j, 1).start()

        @pl.when(r == 1)
        def _():
            extra(j, 7).start()

        @pl.when(r == 3)
        def _():
            up(j, 0, loth.at[j], z).start()

        @pl.when(r == 0)
        def _():
            down(j, 0, loth.at[j], z).start()

        @pl.when(r < 3)
        def _():
            up(j, 0, lbuf.at[j, z], z).start()

        @pl.when(r > 0)
        def _():
            down(j, 0, lbuf.at[j, z], z).start()

    for j in (0, 1):
        launch(j)

    def relay(way):
        t = way
        frm = lax.rem(y + (3 if way == 0 else 1), 4)
        ref = gbuf.at[h, t, :, frm]
        return copy_to(ref, ref, gr_s.at[way], gr_r.at[way], at_y(1 if way == 0 else 3))

    gy(0, 0).wait_recv()
    relay(0).start()
    gy(1, 1).wait_recv()
    relay(1).start()

    def gc(d, t):
        ref = gbuf.at[oth, t, :, y]
        return copy_to(ref, ref, gc_s.at[d - 1, t], gc_r.at[d - 1, t], at_y(d))

    for t in (0, 1):
        gz(t).wait_recv()
        for d in (1, 3, 2):
            gc(d, t).start()

    gy(0, 1).wait_recv()
    gy(1, 0).wait_recv()
    relay(0).wait_recv()
    relay(1).wait_recv()

    def turn(half):
        @pl.loop(0, 4)
        def _(q):
            for t in (0, 1):
                gt[half * 4 + q, t] = gbuf[half, t, q].reshape(4 * E, ROWS).T

    turn(h)

    def compute(slot, j, zp):
        right = lbuf[j, zp].reshape(4 * E, 2 * LN)
        for t in (0, 1):
            acc[slot, t] += dot(gt[zp, t], right)

    def first(j):
        right = lbuf[j, z].reshape(4 * E, 2 * LN)
        for t in (0, 1):
            acc[j, t] = dot(gt[z, t], right)

    def edge(j):
        @pl.when(r == 3)
        def _():
            extra(j, 1).wait_recv()
            up(j, 1, lrel.at[j], 4 * h + 2).start()

        @pl.when(r == 0)
        def _():
            extra(j, 7).wait_recv()
            down(j, 1, lrel.at[j], 4 * h + 1).start()

    def relay_from(j, d):
        zp = lax.rem(z + 7 - d, 8)
        zm = lax.rem(z + 1 + d, 8)

        @pl.when(d < r + 2)
        def _():
            up(j, d, lbuf.at[j, zp], zp).wait_recv()

            if d < 4:
                @pl.when(r < 3)
                def _():
                    up(j, d + 1, lbuf.at[j, zp], zp).start()

        @pl.when(d < 5 - r)
        def _():
            down(j, d, lbuf.at[j, zm], zm).wait_recv()

            if d < 4:
                @pl.when(r > 0)
                def _():
                    down(j, d + 1, lbuf.at[j, zm], zm).start()

    def compute_from(j, d):
        @pl.when(d < r + 2)
        def _():
            compute(j, j, lax.rem(z + 7 - d, 8))

        @pl.when(d < 5 - r)
        def _():
            compute(j, j, lax.rem(z + 1 + d, 8))

    def compute_rest(j):
        @pl.loop(1, 8)
        def _(k):
            compute(j, j, lax.rem(z + k, 8))

    def out_copy(j):
        cols = pl.ds(ORDER[j] * LN, LN)
        return pltpu.make_async_copy(xs.at[:, :, cols], x_out.at[0, :, :, cols], o_s.at[j])

    def finish(slot, j):
        lo = ORDER[j] * LN

        @pl.loop(0, 8)
        def _(b):
            rows = pl.ds(b * E, E)
            re = acc[slot, 1, rows, LN:] - acc[slot, 0, rows, :LN]
            im = -(acc[slot, 0, rows, LN:] + acc[slot, 1, rows, :LN])
            xs[0, rows, lo:lo + LN] = re
            xs[1, rows, lo:lo + LN] = im
            xb[j, rows, :LN] = re.astype(BF16)
            xb[j, rows, LN:] = im.astype(BF16)

        out_copy(j).start()

    def diag(ja, jb):
        low = lbuf[ja, r].reshape(4 * E, 2 * LN)
        high = lbuf[ja, 4 + r].reshape(4 * E, 2 * LN)
        both = dot(low, xb[jb, :4 * E], (0, 0)) + dot(high, xb[jb, 4 * E:], (0, 0))
        lo = ORDER[ja] * LN
        dsend[ORDER[jb], 0, lo:lo + LN] = (both[:LN, :LN] - both[LN:, LN:]).astype(BF16)
        dsend[ORDER[jb], 1, lo:lo + LN] = (both[:LN, LN:] + both[LN:, :LN]).astype(BF16)

    for d in range(5):
        for j in (0, 1):
            if d == 0:
                edge(j)
            relay_from(j, d)
        if d == 2:
            for j in (2, 3):
                launch(j)
    for t in (0, 1):
        for d in (1, 3, 2):
            gc(d, t).wait_recv()
    turn(oth)
    for d in range(5):
        for j in (2, 3):
            if d == 0:
                edge(j)
            relay_from(j, d)
            if d == 0:
                first(j)
            compute_from(j, d)
        if d < 2:
            first(d)
            compute_rest(d)
            finish(d, d)
    finish(2, 2)
    finish(3, 3)

    for jb in range(4):
        for ja in range(4):
            diag(ja, jb)

    def share(d):
        return copy_to(
            dsend.at[lax.rem(r + d, 4)], drecv.at[d - 1], d_s.at[d - 1], d_r.at[d - 1], at_row(d)
        )

    for d in (1, 2, 3):
        share(d).start()
    for d in (1, 2, 3):
        share(d).wait_recv()

    def full(t):
        got = dsend[r, t].astype(F32)
        for d in range(3):
            got += drecv[d, t].astype(F32)
        return d_in[0, t].astype(F32) - got

    re = full(0)
    im = full(1)
    id_out[0, 0] = re.astype(BF16)
    id_out[0, 1] = im.astype(BF16)
    term[...] = wgt[0, 0] * im + wgt[0, 1] * re

    mine = pl.ds(pl.multiple_of(core * 256, 256), 256)
    other = pl.ds(pl.multiple_of((1 - core) * 256, 256), 256)
    pair = copy_to(term.at[other], tpair, t_s, t_r, partner)
    pair.start()
    pair.wait_recv()
    px[xx] = (term[mine, :] + tpair[...]).astype(BF16)

    def along(d):
        return copy_to(px.at[xx], px.at[xx], p_s.at[d - 1], p_r.at[d - 1], at_x(d))

    for d in (1, 3, 2):
        along(d).start()
    for d in (1, 3, 2):
        along(d).wait_recv()
    half = px[0].astype(F32)
    for k in range(1, 4):
        half += px[k].astype(F32)
    dh[...] = half
    den_out[mine, :] = half
    swap = copy_to(dh, dp, h_s, h_r, partner)
    swap.start()
    swap.wait_recv()
    den_out[other, :] = dp[...]

    for t in (0, 1):
        gz(t).wait_send()
        gy(0, t).wait_send()
        gy(1, t).wait_send()
        relay(t).wait_send()
        for d in (1, 2, 3):
            gc(d, t).wait_send()
            to_col(d, t).wait_send()
    for d in (1, 2, 3):
        share(d).wait_send()
        along(d).wait_send()
    pair.wait_send()
    swap.wait_send()

    @pl.loop(0, 4)
    def _(j):
        @pl.when((r == 1) | (r == 2))
        def _():
            extra(j, 1).wait_send()

        @pl.loop(0, 5)
        def _(i):
            @pl.when(((r < 3) & (i < r + 3)) | ((r == 3) & (i < 2)))
            def _():
                up(j, i, lbuf.at[j, z], z).wait_send()

            @pl.when(((r > 0) & (i < 6 - r)) | ((r == 0) & (i < 2)))
            def _():
                down(j, i, lbuf.at[j, z], z).wait_send()

    for j in range(4):
        out_copy(j).wait()


def body(anc_inverse, panel, pattern, diag_inverse, pole_weights):
    vmem = pl.BlockSpec(memory_space=pltpu.VMEM)
    smem = pl.BlockSpec(memory_space=pltpu.SMEM)
    dma = pltpu.SemaphoreType.DMA
    sems = [(3, 2), (2,), (2, 2), (2,), (3, 2), (4, 5), (4, 5), (4,), (3,), None, (3,), None]
    pairs = []
    for shape in sems:
        one = dma if shape is None else dma(shape)
        pairs += [one, one]
    return pl.pallas_call(
        kernel,
        out_shape=(
            jax.ShapeDtypeStruct((1, 2, ROWS, 512), F32),
            jax.ShapeDtypeStruct((1, 2, 512, LN), BF16),
            jax.ShapeDtypeStruct((512, LN), F32),
        ),
        in_specs=[smem, smem, vmem, vmem, vmem],
        out_specs=(pl.BlockSpec(memory_space=pl.ANY), vmem, vmem),
        scratch_shapes=[
            pltpu.VMEM((2, 2, 4, 4, E, ROWS), BF16),
            pltpu.VMEM((8, 2, ROWS, 4 * E), BF16),
            pltpu.VMEM((8, 4, E, 2 * LN), BF16),
            pltpu.VMEM((4, 8, 4, E, 2 * LN), BF16),
            pltpu.VMEM((4, 4, E, 2 * LN), BF16),
            pltpu.VMEM((4, 4, E, 2 * LN), BF16),
            pltpu.VMEM((4, 2, ROWS, 2 * LN), F32),
            pltpu.VMEM((2, ROWS, 512), F32),
            pltpu.VMEM((4, ROWS, 2 * LN), BF16),
            pltpu.VMEM((4, 2, 512, LN), BF16),
            pltpu.VMEM((3, 2, 512, LN), BF16),
            pltpu.VMEM((512, LN), F32),
            pltpu.VMEM((256, LN), F32),
            pltpu.VMEM((4, 256, LN), BF16),
            pltpu.VMEM((256, LN), F32),
            pltpu.VMEM((256, LN), F32),
            *pairs,
            dma((4,)),
        ],
        compiler_params=pltpu.CompilerParams(
            collective_id=0, has_side_effects=True, vmem_limit_bytes=60 * 1024 * 1024
        ),
    )(pattern.T, pole_weights, anc_inverse, panel, diag_inverse)


def solution(mesh):
    placed = (
        P("pole", None, None, "col", "row"),
        P("pole", None, ("row", "col"), None),
        P(),
        P("pole", None, "col", "row"),
        P("pole", None),
    )
    return jax.shard_map(
        body,
        mesh=mesh,
        in_specs=placed,
        out_specs=(P("pole", None, "row", "col"), P("pole", None, "col", "row"), P("col", "row")),
        check_vma=False,
    )
```

```python
import jax
import jax.numpy as jnp
from jax import lax
from jax.experimental import pallas as pl
from jax.experimental.pallas import tpu as pltpu
from jax.sharding import PartitionSpec as P

MESH = pl.DeviceIdType.MESH
F32 = jnp.float32
BF16 = jnp.bfloat16

E = 96
ROWS = 768
LN = 128
ORDER = (1, 2, 0, 3)


def copy_to(src, dst, send_sem, recv_sem, dev):
    return pltpu.make_async_remote_copy(
        src_ref=src,
        dst_ref=dst,
        send_sem=send_sem,
        recv_sem=recv_sem,
        device_id=dev,
        device_id_type=MESH,
    )


def dot(a, b, dims=(1, 0)):
    return lax.dot_general(
        a, b, (((dims[0],), (dims[1],)), ((), ())), preferred_element_type=F32
    )


def kernel(
    pat, wgt, g_in, p_in, d_in,
    x_out, id_out, den_out,
    gbuf, gt, lsrc, lbuf, loth, lrel, acc, xs, xb, dsend, drecv, term, tpair, px, dh, dp,
    a_s, a_r, gz_s, gz_r, gy_s, gy_r, gr_s, gr_r, gc_s, gc_r,
    lp_s, lp_r, lm_s, lm_r, x_s, x_r, d_s, d_r, t_s, t_r, p_s, p_r, h_s, h_r, o_s,
):
    pole = lax.axis_index("pole")
    r = lax.axis_index("row")
    c = lax.axis_index("col")
    h = c // 4
    y = lax.rem(c, 4)
    z = 4 * h + r
    oth = 1 - h
    core = lax.rem(pole, 2)
    xx = pole // 2

    def at_y(d):
        return {"col": 4 * h + lax.rem(y + d, 4)}

    def at_z(d):
        zz = lax.rem(z + d, 8)
        return {"row": lax.rem(zz, 4), "col": (zz // 4) * 4 + y}

    def at_row(d):
        return {"row": lax.rem(r + d, 4)}

    def at_x(d):
        return {"pole": lax.rem(xx + d, 4) * 2 + core}

    partner = {"pole": 2 * xx + 1 - core}
    across = {"col": 4 * oth + y}

    bar = pltpu.get_barrier_semaphore()
    peers = [at_y(1), at_y(2), at_y(3), at_z(1), at_z(7), across, partner]
    peers += [at_row(d) for d in (1, 2, 3)] + [at_x(d) for d in (1, 2, 3)]
    for dev in peers:
        pl.semaphore_signal(bar, inc=1, device_id=dev, device_id_type=MESH)
    pl.semaphore_wait(bar, len(peers))

    def gz(t):
        return copy_to(g_in.at[0, t], gbuf.at[h, t, :, y], gz_s.at[t], gz_r.at[t], across)

    for t in (0, 1):
        gz(t).start()

    fine = r * 8 + c
    for k in range(8):
        keep = pat[k, fine].astype(F32)
        for j in range(4):
            lo = k * 512 + ORDER[j] * LN
            for t in (0, 1):
                blk = p_in[0, t, :, lo:lo + LN].astype(F32) * keep
                lsrc[k, j, :, t * LN:(t + 1) * LN] = blk.astype(BF16)
    gbuf[h, :, :, y] = g_in[0]

    def to_col(d, which):
        k = (h if which == 0 else oth) * 4 + lax.rem(y + d, 4)
        dst = lbuf.at[:, z, y] if which == 0 else loth.at[:, y]
        return copy_to(lsrc.at[k], dst, a_s.at[d - 1, which], a_r.at[d - 1, which], at_y(d))

    for which in (1, 0):
        for d in (1, 3, 2):
            to_col(d, which).start()

    def gy(way, t):
        return copy_to(
            g_in.at[0, t], gbuf.at[h, t, :, y], gy_s.at[way, t], gy_r.at[way, t], at_y(1 if way == 0 else 3)
        )

    for i in (0, 1):
        gy(0, i).start()
        gy(1, 1 - i).start()

    lbuf[:, z, y] = lsrc[h * 4 + y]
    loth[:, y] = lsrc[oth * 4 + y]

    for which in (1, 0):
        for d in (1, 3, 2):
            to_col(d, which).wait_recv()

    def up(j, i, src, zp):
        return copy_to(src, lbuf.at[j, zp], lp_s.at[j, i], lp_r.at[j, i], at_z(1))

    def down(j, i, src, zp):
        return copy_to(src, lbuf.at[j, zp], lm_s.at[j, i], lm_r.at[j, i], at_z(7))

    def extra(j, d):
        return copy_to(loth.at[j], lrel.at[j], x_s.at[j], x_r.at[j], at_z(d))

    def launch(j):
        @pl.when(r == 2)
        def _():
            extra(j, 1).start()

        @pl.when(r == 1)
        def _():
            extra(j, 7).start()

        @pl.when(r == 3)
        def _():
            up(j, 0, loth.at[j], z).start()

        @pl.when(r == 0)
        def _():
            down(j, 0, loth.at[j], z).start()

        @pl.when(r < 3)
        def _():
            up(j, 0, lbuf.at[j, z], z).start()

        @pl.when(r > 0)
        def _():
            down(j, 0, lbuf.at[j, z], z).start()

    for j in (0, 1):
        launch(j)

    def relay(way):
        t = way
        frm = lax.rem(y + (3 if way == 0 else 1), 4)
        ref = gbuf.at[h, t, :, frm]
        return copy_to(ref, ref, gr_s.at[way], gr_r.at[way], at_y(1 if way == 0 else 3))

    gy(0, 0).wait_recv()
    relay(0).start()
    gy(1, 1).wait_recv()
    relay(1).start()

    def gc(d, t):
        ref = gbuf.at[oth, t, :, y]
        return copy_to(ref, ref, gc_s.at[d - 1, t], gc_r.at[d - 1, t], at_y(d))

    for t in (0, 1):
        gz(t).wait_recv()
        for d in (1, 3, 2):
            gc(d, t).start()

    gy(0, 1).wait_recv()
    gy(1, 0).wait_recv()
    relay(0).wait_recv()
    relay(1).wait_recv()

    def turn(half):
        @pl.loop(0, 4)
        def _(q):
            for t in (0, 1):
                gt[half * 4 + q, t] = gbuf[half, t, q].reshape(4 * E, ROWS).T

    turn(h)

    def compute(slot, j, zp):
        right = lbuf[j, zp].reshape(4 * E, 2 * LN)
        for t in (0, 1):
            acc[slot, t] += dot(gt[zp, t], right)

    def first(j):
        right = lbuf[j, z].reshape(4 * E, 2 * LN)
        for t in (0, 1):
            acc[j, t] = dot(gt[z, t], right)

    def edge(j):
        @pl.when(r == 3)
        def _():
            extra(j, 1).wait_recv()
            up(j, 1, lrel.at[j], 4 * h + 2).start()

        @pl.when(r == 0)
        def _():
            extra(j, 7).wait_recv()
            down(j, 1, lrel.at[j], 4 * h + 1).start()

    def relay_from(j, d):
        zp = lax.rem(z + 7 - d, 8)
        zm = lax.rem(z + 1 + d, 8)

        @pl.when(d < r + 2)
        def _():
            up(j, d, lbuf.at[j, zp], zp).wait_recv()

            if d < 4:
                @pl.when(r < 3)
                def _():
                    up(j, d + 1, lbuf.at[j, zp], zp).start()

        @pl.when(d < 5 - r)
        def _():
            down(j, d, lbuf.at[j, zm], zm).wait_recv()

            if d < 4:
                @pl.when(r > 0)
                def _():
                    down(j, d + 1, lbuf.at[j, zm], zm).start()

    def compute_from(j, d):
        @pl.when(d < r + 2)
        def _():
            compute(j, j, lax.rem(z + 7 - d, 8))

        @pl.when(d < 5 - r)
        def _():
            compute(j, j, lax.rem(z + 1 + d, 8))

    def compute_rest(j):
        @pl.loop(1, 8)
        def _(k):
            compute(j, j, lax.rem(z + k, 8))

    def out_copy(j):
        cols = pl.ds(ORDER[j] * LN, LN)
        return pltpu.make_async_copy(xs.at[:, :, cols], x_out.at[0, :, :, cols], o_s.at[j])

    def finish(slot, j):
        lo = ORDER[j] * LN

        @pl.loop(0, 8)
        def _(b):
            rows = pl.ds(b * E, E)
            re = acc[slot, 1, rows, LN:] - acc[slot, 0, rows, :LN]
            im = -(acc[slot, 0, rows, LN:] + acc[slot, 1, rows, :LN])
            xs[0, rows, lo:lo + LN] = re
            xs[1, rows, lo:lo + LN] = im
            xb[j, rows, :LN] = re.astype(BF16)
            xb[j, rows, LN:] = im.astype(BF16)

        out_copy(j).start()

    def diag(ja, jb):
        low = lbuf[ja, r].reshape(4 * E, 2 * LN)
        high = lbuf[ja, 4 + r].reshape(4 * E, 2 * LN)
        both = dot(low, xb[jb, :4 * E], (0, 0)) + dot(high, xb[jb, 4 * E:], (0, 0))
        lo = ORDER[ja] * LN
        dsend[ORDER[jb], 0, lo:lo + LN] = (both[:LN, :LN] - both[LN:, LN:]).astype(BF16)
        dsend[ORDER[jb], 1, lo:lo + LN] = (both[:LN, LN:] + both[LN:, :LN]).astype(BF16)

    for d in range(5):
        for j in (0, 1):
            if d == 0:
                edge(j)
            relay_from(j, d)
        if d == 2:
            for j in (2, 3):
                launch(j)
    for t in (0, 1):
        for d in (1, 3, 2):
            gc(d, t).wait_recv()
    turn(oth)
    def share(j):
        own = ORDER[j]
        d = lax.rem(own + 4 - r, 4) - 1
        slot = jnp.maximum(d, 0)
        return copy_to(dsend.at[own], drecv.at[slot], d_s.at[slot], d_r.at[slot], {"row": own})

    def give(j):
        @pl.when(r != ORDER[j])
        def _():
            share(j).start()

    for d in range(5):
        for j in (2, 3):
            if d == 0:
                edge(j)
            relay_from(j, d)
            if d == 0:
                first(j)
            compute_from(j, d)
        if d < 2:
            first(d)
            compute_rest(d)
            finish(d, d)
        if d == 2:
            for jb in (0, 1):
                for ja in (0, 1):
                    diag(ja, jb)
        if d == 3:
            for jb in (0, 1):
                for ja in (2, 3):
                    diag(ja, jb)
            give(0)
            give(1)
    finish(2, 2)
    for ja in range(4):
        diag(ja, 2)
    finish(3, 3)
    give(2)
    for ja in range(4):
        diag(ja, 3)
    give(3)

    for d in range(3):
        copy_to(dsend.at[r], drecv.at[d], d_s.at[d], d_r.at[d], partner).wait_recv()

    def full(t):
        got = dsend[r, t].astype(F32)
        for d in range(3):
            got += drecv[d, t].astype(F32)
        return d_in[0, t].astype(F32) - got

    re = full(0)
    im = full(1)
    id_out[0, 0] = re.astype(BF16)
    id_out[0, 1] = im.astype(BF16)
    term[...] = wgt[0, 0] * im + wgt[0, 1] * re

    mine = pl.ds(pl.multiple_of(core * 256, 256), 256)
    other = pl.ds(pl.multiple_of((1 - core) * 256, 256), 256)
    pair = copy_to(term.at[other], tpair, t_s, t_r, partner)
    pair.start()
    pair.wait_recv()
    px[xx] = (term[mine, :] + tpair[...]).astype(BF16)

    def along(d):
        return copy_to(px.at[xx], px.at[xx], p_s.at[d - 1], p_r.at[d - 1], at_x(d))

    for d in (1, 3, 2):
        along(d).start()
    for d in (1, 3, 2):
        along(d).wait_recv()
    half = px[0].astype(F32)
    for k in range(1, 4):
        half += px[k].astype(F32)
    dh[...] = half
    den_out[mine, :] = half
    swap = copy_to(dh, dp, h_s, h_r, partner)
    swap.start()
    swap.wait_recv()
    den_out[other, :] = dp[...]

    for t in (0, 1):
        gz(t).wait_send()
        gy(0, t).wait_send()
        gy(1, t).wait_send()
        relay(t).wait_send()
        for d in (1, 2, 3):
            gc(d, t).wait_send()
            to_col(d, t).wait_send()
    for j in range(4):
        @pl.when(r != ORDER[j])
        def _():
            share(j).wait_send()

    for d in (1, 2, 3):
        along(d).wait_send()
    pair.wait_send()
    swap.wait_send()

    @pl.loop(0, 4)
    def _(j):
        @pl.when((r == 1) | (r == 2))
        def _():
            extra(j, 1).wait_send()

        @pl.loop(0, 5)
        def _(i):
            @pl.when(((r < 3) & (i < r + 3)) | ((r == 3) & (i < 2)))
            def _():
                up(j, i, lbuf.at[j, z], z).wait_send()

            @pl.when(((r > 0) & (i < 6 - r)) | ((r == 0) & (i < 2)))
            def _():
                down(j, i, lbuf.at[j, z], z).wait_send()

    for j in range(4):
        out_copy(j).wait()


def body(anc_inverse, panel, pattern, diag_inverse, pole_weights):
    vmem = pl.BlockSpec(memory_space=pltpu.VMEM)
    smem = pl.BlockSpec(memory_space=pltpu.SMEM)
    dma = pltpu.SemaphoreType.DMA
    sems = [(3, 2), (2,), (2, 2), (2,), (3, 2), (4, 5), (4, 5), (4,), (3,), None, (3,), None]
    pairs = []
    for shape in sems:
        one = dma if shape is None else dma(shape)
        pairs += [one, one]
    return pl.pallas_call(
        kernel,
        out_shape=(
            jax.ShapeDtypeStruct((1, 2, ROWS, 512), F32),
            jax.ShapeDtypeStruct((1, 2, 512, LN), BF16),
            jax.ShapeDtypeStruct((512, LN), F32),
        ),
        in_specs=[smem, smem, vmem, vmem, vmem],
        out_specs=(pl.BlockSpec(memory_space=pl.ANY), vmem, vmem),
        scratch_shapes=[
            pltpu.VMEM((2, 2, 4, 4, E, ROWS), BF16),
            pltpu.VMEM((8, 2, ROWS, 4 * E), BF16),
            pltpu.VMEM((8, 4, E, 2 * LN), BF16),
            pltpu.VMEM((4, 8, 4, E, 2 * LN), BF16),
            pltpu.VMEM((4, 4, E, 2 * LN), BF16),
            pltpu.VMEM((4, 4, E, 2 * LN), BF16),
            pltpu.VMEM((4, 2, ROWS, 2 * LN), F32),
            pltpu.VMEM((2, ROWS, 512), F32),
            pltpu.VMEM((4, ROWS, 2 * LN), BF16),
            pltpu.VMEM((4, 2, 512, LN), BF16),
            pltpu.VMEM((3, 2, 512, LN), BF16),
            pltpu.VMEM((512, LN), F32),
            pltpu.VMEM((256, LN), F32),
            pltpu.VMEM((4, 256, LN), BF16),
            pltpu.VMEM((256, LN), F32),
            pltpu.VMEM((256, LN), F32),
            *pairs,
            dma((4,)),
        ],
        compiler_params=pltpu.CompilerParams(
            collective_id=0, has_side_effects=True, vmem_limit_bytes=60 * 1024 * 1024
        ),
    )(pattern.T, pole_weights, anc_inverse, panel, diag_inverse)


def solution(mesh):
    placed = (
        P("pole", None, None, "col", "row"),
        P("pole", None, ("row", "col"), None),
        P(),
        P("pole", None, "col", "row"),
        P("pole", None),
    )
    return jax.shard_map(
        body,
        mesh=mesh,
        in_specs=placed,
        out_specs=(P("pole", None, "row", "col"), P("pole", None, "col", "row"), P("col", "row")),
        check_vma=False,
    )
```

```python
import jax
import jax.numpy as jnp
from jax import lax
from jax.experimental import pallas as pl
from jax.experimental.pallas import tpu as pltpu
from jax.sharding import PartitionSpec as P

MESH = pl.DeviceIdType.MESH
F32 = jnp.float32
BF16 = jnp.bfloat16

E = 96
ROWS = 768
LN = 128
ORDER = (1, 2, 0, 3)


def copy_to(src, dst, send_sem, recv_sem, dev):
    return pltpu.make_async_remote_copy(
        src_ref=src,
        dst_ref=dst,
        send_sem=send_sem,
        recv_sem=recv_sem,
        device_id=dev,
        device_id_type=MESH,
    )


def dot(a, b, dims=(1, 0)):
    return lax.dot_general(
        a, b, (((dims[0],), (dims[1],)), ((), ())), preferred_element_type=F32
    )


def kernel(
    pat, wgt, g_hbm, p_hbm, d_hbm,
    x_out, id_out, den_out,
    g_in, p_in, d_in, gbuf, gt, lsrc, lbuf, loth, lrel, acc, xs, xb, dsend, drecv, way, term, tpair, px, dh, dp,
    a_s, a_r, gz_s, gz_r, gy_s, gy_r, gr_s, gr_r, gc_s, gc_r,
    lp_s, lp_r, lm_s, lm_r, x_s, x_r, d_s, d_r, t_s, t_r, p_s, p_r, h_s, h_r, k_s, k_r, o_s, i_s,
):
    pole = lax.axis_index("pole")
    r = lax.axis_index("row")
    c = lax.axis_index("col")
    h = c // 4
    y = lax.rem(c, 4)
    z = 4 * h + r
    oth = 1 - h
    core = lax.rem(pole, 2)
    xx = pole // 2

    def at_y(d):
        return {"col": 4 * h + lax.rem(y + d, 4)}

    def at_z(d):
        zz = lax.rem(z + d, 8)
        return {"row": lax.rem(zz, 4), "col": (zz // 4) * 4 + y}

    def at_row(d):
        return {"row": lax.rem(r + d, 4)}

    def at_x(d):
        return {"pole": lax.rem(xx + d, 4) * 2 + core}

    partner = {"pole": 2 * xx + 1 - core}
    across = {"col": 4 * oth + y}

    loads = [
        pltpu.make_async_copy(src, dst, i_s.at[i])
        for i, (src, dst) in enumerate(((g_hbm, g_in), (p_hbm, p_in), (d_hbm, d_in)))
    ]
    for load in loads:
        load.start()

    bar = pltpu.get_barrier_semaphore()
    peers = [at_y(1), at_y(2), at_y(3), at_z(1), at_z(7), across, partner]
    peers += [at_row(d) for d in (1, 2, 3)] + [at_x(d) for d in (1, 2, 3)]
    for dev in peers:
        pl.semaphore_signal(bar, inc=1, device_id=dev, device_id_type=MESH)
    loads[0].wait()
    pl.semaphore_wait(bar, len(peers))

    def gz(t):
        return copy_to(g_in.at[0, t], gbuf.at[h, t, :, y], gz_s.at[t], gz_r.at[t], across)

    for t in (0, 1):
        gz(t).start()
    for load in loads[1:]:
        load.wait()

    @pl.when((r == 0) | (r == 3))
    def _():
        drecv[1] = jnp.zeros((2, 512, LN), BF16)

    fine = r * 8 + c
    for k in range(8):
        keep = pat[k, fine].astype(F32)
        for j in range(4):
            lo = k * 512 + ORDER[j] * LN
            for t in (0, 1):
                blk = p_in[0, t, :, lo:lo + LN].astype(F32) * keep
                lsrc[k, j, :, t * LN:(t + 1) * LN] = blk.astype(BF16)
    gbuf[h, :, :, y] = g_in[0]

    def to_col(d, which):
        k = (h if which == 0 else oth) * 4 + lax.rem(y + d, 4)
        dst = lbuf.at[:, z, y] if which == 0 else loth.at[:, y]
        return copy_to(lsrc.at[k], dst, a_s.at[d - 1, which], a_r.at[d - 1, which], at_y(d))

    for which in (1, 0):
        for d in (1, 3, 2):
            to_col(d, which).start()

    def gy(way, t):
        return copy_to(
            g_in.at[0, t], gbuf.at[h, t, :, y], gy_s.at[way, t], gy_r.at[way, t], at_y(1 if way == 0 else 3)
        )

    for i in (0, 1):
        gy(0, i).start()
        gy(1, 1 - i).start()

    lbuf[:, z, y] = lsrc[h * 4 + y]
    loth[:, y] = lsrc[oth * 4 + y]

    for which in (1, 0):
        for d in (1, 3, 2):
            to_col(d, which).wait_recv()

    def up(j, i, src, zp):
        return copy_to(src, lbuf.at[j, zp], lp_s.at[j, i], lp_r.at[j, i], at_z(1))

    def down(j, i, src, zp):
        return copy_to(src, lbuf.at[j, zp], lm_s.at[j, i], lm_r.at[j, i], at_z(7))

    def extra(j, d):
        return copy_to(loth.at[j], lrel.at[j], x_s.at[j], x_r.at[j], at_z(d))

    def launch_far(j):
        @pl.when(r == 2)
        def _():
            extra(j, 1).start()

        @pl.when(r == 1)
        def _():
            extra(j, 7).start()

        @pl.when(r == 3)
        def _():
            up(j, 0, loth.at[j], z).start()

        @pl.when(r == 0)
        def _():
            down(j, 0, loth.at[j], z).start()

    def launch(j):
        @pl.when(r < 3)
        def _():
            up(j, 0, lbuf.at[j, z], z).start()

        @pl.when(r > 0)
        def _():
            down(j, 0, lbuf.at[j, z], z).start()

    for j in range(4):
        launch_far(j)
    for j in (0, 1):
        launch(j)

    def relay(way):
        t = way
        frm = lax.rem(y + (3 if way == 0 else 1), 4)
        ref = gbuf.at[h, t, :, frm]
        return copy_to(ref, ref, gr_s.at[way], gr_r.at[way], at_y(1 if way == 0 else 3))

    gy(0, 0).wait_recv()
    relay(0).start()
    gy(1, 1).wait_recv()
    relay(1).start()

    def gc(d, t):
        ref = gbuf.at[oth, t, :, y]
        return copy_to(ref, ref, gc_s.at[d - 1, t], gc_r.at[d - 1, t], at_y(d))

    for t in (0, 1):
        gz(t).wait_recv()
        for d in (1, 3, 2):
            gc(d, t).start()

    gy(0, 1).wait_recv()
    gy(1, 0).wait_recv()
    relay(0).wait_recv()
    relay(1).wait_recv()

    def turn(half):
        @pl.loop(0, 4)
        def _(q):
            for t in (0, 1):
                gt[half * 4 + q, t] = gbuf[half, t, q].reshape(4 * E, ROWS).T

    turn(h)

    def compute(slot, j, zp):
        right = lbuf[j, zp].reshape(4 * E, 2 * LN)
        for t in (0, 1):
            acc[slot, t] += dot(gt[zp, t], right)

    def first(j):
        right = lbuf[j, z].reshape(4 * E, 2 * LN)
        for t in (0, 1):
            acc[j, t] = dot(gt[z, t], right)

    def edge(j):
        @pl.when(r == 3)
        def _():
            extra(j, 1).wait_recv()
            up(j, 1, lrel.at[j], 4 * h + 2).start()

        @pl.when(r == 0)
        def _():
            extra(j, 7).wait_recv()
            down(j, 1, lrel.at[j], 4 * h + 1).start()

    def relay_up(j, d, live=True):
        zp = lax.rem(z + 7 - d, 8)

        @pl.when((d < r + 2) & live)
        def _():
            up(j, d, lbuf.at[j, zp], zp).wait_recv()

            if d < 4:
                @pl.when(r < 3)
                def _():
                    up(j, d + 1, lbuf.at[j, zp], zp).start()

    def relay_down(j, d, live=True):
        zm = lax.rem(z + 1 + d, 8)

        @pl.when((d < 5 - r) & live)
        def _():
            down(j, d, lbuf.at[j, zm], zm).wait_recv()

            if d < 4:
                @pl.when(r > 0)
                def _():
                    down(j, d + 1, lbuf.at[j, zm], zm).start()

    def compute_up(j, d):
        @pl.when(d < r + 2)
        def _():
            compute(j, j, lax.rem(z + 7 - d, 8))

    def compute_down(j, d):
        @pl.when(d < 5 - r)
        def _():
            compute(j, j, lax.rem(z + 1 + d, 8))

    def compute_rest(j):
        @pl.loop(1, 8)
        def _(k):
            compute(j, j, lax.rem(z + k, 8))

    def out_copy(j):
        cols = pl.ds(ORDER[j] * LN, LN)
        return pltpu.make_async_copy(xs.at[:, :, cols], x_out.at[0, :, :, cols], o_s.at[j])

    def finish(slot, j):
        lo = ORDER[j] * LN

        @pl.loop(0, 8)
        def _(b):
            rows = pl.ds(b * E, E)
            re = acc[slot, 1, rows, LN:] - acc[slot, 0, rows, :LN]
            im = -(acc[slot, 0, rows, LN:] + acc[slot, 1, rows, :LN])
            xs[0, rows, lo:lo + LN] = re
            xs[1, rows, lo:lo + LN] = im
            xb[j, rows, :LN] = re.astype(BF16)
            xb[j, rows, LN:] = im.astype(BF16)

        out_copy(j).start()

    def diag(jb, start=0, stop=4):
        @pl.loop(start, stop)
        def _(ja):
            low = lbuf[ja, r].reshape(4 * E, 2 * LN)
            high = lbuf[ja, 4 + r].reshape(4 * E, 2 * LN)
            both = dot(low, xb[jb, :4 * E], (0, 0)) + dot(high, xb[jb, 4 * E:], (0, 0))
            rows = pl.ds(pl.multiple_of(ja * LN, LN), LN)
            dsend[ORDER[jb], 0, rows, :] = (both[:LN, :LN] - both[LN:, LN:]).astype(BF16)
            dsend[ORDER[jb], 1, rows, :] = (both[:LN, LN:] + both[LN:, :LN]).astype(BF16)

    for d in range(5):
        for j in (0, 1):
            if d == 0:
                edge(j)
            relay_up(j, d)
            relay_down(j, d)
        if d == 2:
            for j in (2, 3):
                launch(j)
                edge(j)
            for i in (0, 1):
                for j in (2, 3):
                    relay_up(j, i, r == 0)
                    relay_down(j, i, r == 3)
    def share(j, part):
        own = ORDER[j]
        d = lax.rem(own + 4 - r, 4) - 1
        slot = jnp.maximum(d, 0)
        rows = pl.ds(part * 2 * LN, 2 * LN)
        return copy_to(
            dsend.at[own, :, rows], drecv.at[slot, :, rows], d_s.at[slot, part], d_r.at[slot, part], {"row": own}
        )

    def give(j, part):
        @pl.when(r != ORDER[j])
        def _():
            share(j, part).start()

    def give_both(j):
        share(j, 0).start()
        share(j, 1).start()

    for d in range(5):
        relay_up(2, d, r > 0)
        relay_down(3, d, r < 3)
        if d > 0:
            relay_up(3, d - 1, r > 0)
            relay_down(2, d - 1, r < 3)
        if d == 0:
            continue
        if d == 1:
            for t in (0, 1):
                for i in (1, 3, 2):
                    gc(i, t).wait_recv()
            turn(oth)
            first(2)
            first(3)
            compute_up(2, 0)
            compute_down(3, 0)
        compute_up(2, d)
        compute_down(3, d)
        compute_up(3, d - 1)
        compute_down(2, d - 1)
        if d < 3:
            first(d - 1)
            compute_rest(d - 1)
            finish(d - 1, d - 1)
        if d == 2:
            diag(0, 0, 2)
            diag(1, 0, 2)
            give(0, 0)
            give(1, 0)
        if d == 4:
            diag(0, 2, 4)
            diag(1, 2, 4)
            give(0, 1)
            give(1, 1)

    @pl.when(r > 0)
    def _():
        finish(2, 2)
        diag(2)

    @pl.when(r < 3)
    def _():
        finish(3, 3)
        diag(3)

    def meet(own):
        return copy_to(dsend.at[own], way, k_s, k_r, {"row": 3 - r})

    def pass_on(own, j):
        meet(3 - own).start()
        meet(own).wait_recv()
        for t in (0, 1):
            dsend[own, t] = (dsend[own, t].astype(F32) + way[t].astype(F32)).astype(BF16)
        give_both(j)

    @pl.when(r == 1)
    def _():
        pass_on(0, 2)

    @pl.when(r == 2)
    def _():
        pass_on(3, 3)

    @pl.when(r == 3)
    def _():
        give_both(2)
        relay_up(3, 4)
        compute_up(3, 4)
        finish(3, 3)
        diag(3)

    @pl.when(r == 0)
    def _():
        give_both(3)
        relay_down(2, 4)
        compute_down(2, 4)
        finish(2, 2)
        diag(2)

    def got(d, part):
        rows = pl.ds(part * 2 * LN, 2 * LN)
        return copy_to(
            dsend.at[r, :, rows], drecv.at[d, :, rows], d_s.at[d, part], d_r.at[d, part], partner
        )

    for part in (0, 1):
        got(0, part).wait_recv()
        got(2, part).wait_recv()

        @pl.when((r == 1) | (r == 2))
        def _():
            got(1, part).wait_recv()

    for j in range(4):
        rows = pl.ds(j * LN, LN)
        cols = pl.ds(ORDER[j] * LN, LN)
        part = []
        for t in (0, 1):
            sum_ = dsend[r, t, rows, :].astype(F32)
            for d in range(3):
                sum_ += drecv[d, t, rows, :].astype(F32)
            part.append(d_in[0, t, cols, :].astype(F32) - sum_)
            id_out[0, t, cols, :] = part[t].astype(BF16)
        term[cols, :] = wgt[0, 0] * part[1] + wgt[0, 1] * part[0]

    mine = pl.ds(pl.multiple_of(core * 256, 256), 256)
    other = pl.ds(pl.multiple_of((1 - core) * 256, 256), 256)
    pair = copy_to(term.at[other], tpair, t_s, t_r, partner)
    pair.start()
    pair.wait_recv()
    px[xx] = (term[mine, :] + tpair[...]).astype(BF16)

    def along(d):
        return copy_to(px.at[xx], px.at[xx], p_s.at[d - 1], p_r.at[d - 1], at_x(d))

    for d in (1, 3, 2):
        along(d).start()
    for d in (1, 3, 2):
        along(d).wait_recv()
    half = px[0].astype(F32)
    for k in range(1, 4):
        half += px[k].astype(F32)
    dh[...] = half
    den_out[mine, :] = half
    swap = copy_to(dh, dp, h_s, h_r, partner)
    swap.start()
    swap.wait_recv()
    den_out[other, :] = dp[...]

    for t in (0, 1):
        gz(t).wait_send()
        gy(0, t).wait_send()
        gy(1, t).wait_send()
        relay(t).wait_send()
        for d in (1, 2, 3):
            gc(d, t).wait_send()
            to_col(d, t).wait_send()
    for j in (0, 1):
        @pl.when(r != ORDER[j])
        def _():
            for part in (0, 1):
                share(j, part).wait_send()

    for part in (0, 1):
        @pl.when((r == 1) | (r == 3))
        def _():
            share(2, part).wait_send()

        @pl.when((r == 0) | (r == 2))
        def _():
            share(3, part).wait_send()

    @pl.when((r == 1) | (r == 2))
    def _():
        meet(0).wait_send()

    for d in (1, 2, 3):
        along(d).wait_send()
    pair.wait_send()
    swap.wait_send()

    @pl.loop(0, 4)
    def _(j):
        @pl.when((r == 1) | (r == 2))
        def _():
            extra(j, 1).wait_send()

        @pl.loop(0, 5)
        def _(i):
            @pl.when(((r < 3) & (i < r + 3)) | ((r == 3) & (i < 2)))
            def _():
                up(j, i, lbuf.at[j, z], z).wait_send()

            @pl.when(((r > 0) & (i < 6 - r)) | ((r == 0) & (i < 2)))
            def _():
                down(j, i, lbuf.at[j, z], z).wait_send()

    for j in range(4):
        out_copy(j).wait()


def body(anc_inverse, panel, pattern, diag_inverse, pole_weights):
    vmem = pl.BlockSpec(memory_space=pltpu.VMEM)
    hbm = pl.BlockSpec(memory_space=pl.ANY)
    smem = pl.BlockSpec(memory_space=pltpu.SMEM)
    dma = pltpu.SemaphoreType.DMA
    sems = [(3, 2), (2,), (2, 2), (2,), (3, 2), (4, 5), (4, 5), (4,), (3, 2), None, (3,), None, None]
    pairs = []
    for shape in sems:
        one = dma if shape is None else dma(shape)
        pairs += [one, one]
    return pl.pallas_call(
        kernel,
        out_shape=(
            jax.ShapeDtypeStruct((1, 2, ROWS, 512), F32),
            jax.ShapeDtypeStruct((1, 2, 512, LN), BF16),
            jax.ShapeDtypeStruct((512, LN), F32),
        ),
        in_specs=[smem, smem, hbm, hbm, hbm],
        out_specs=(hbm, vmem, vmem),
        scratch_shapes=[
            pltpu.VMEM((1, 2, 4, E, ROWS), BF16),
            pltpu.VMEM((1, 2, E, 4096), BF16),
            pltpu.VMEM((1, 2, 512, LN), BF16),
            pltpu.VMEM((2, 2, 4, 4, E, ROWS), BF16),
            pltpu.VMEM((8, 2, ROWS, 4 * E), BF16),
            pltpu.VMEM((8, 4, E, 2 * LN), BF16),
            pltpu.VMEM((4, 8, 4, E, 2 * LN), BF16),
            pltpu.VMEM((4, 4, E, 2 * LN), BF16),
            pltpu.VMEM((4, 4, E, 2 * LN), BF16),
            pltpu.VMEM((4, 2, ROWS, 2 * LN), F32),
            pltpu.VMEM((2, ROWS, 512), F32),
            pltpu.VMEM((4, ROWS, 2 * LN), BF16),
            pltpu.VMEM((4, 2, 512, LN), BF16),
            pltpu.VMEM((3, 2, 512, LN), BF16),
            pltpu.VMEM((2, 512, LN), BF16),
            pltpu.VMEM((512, LN), F32),
            pltpu.VMEM((256, LN), F32),
            pltpu.VMEM((4, 256, LN), BF16),
            pltpu.VMEM((256, LN), F32),
            pltpu.VMEM((256, LN), F32),
            *pairs,
            dma((4,)),
            dma((3,)),
        ],
        compiler_params=pltpu.CompilerParams(
            collective_id=0, has_side_effects=True, vmem_limit_bytes=60 * 1024 * 1024
        ),
    )(pattern.T, pole_weights, anc_inverse, panel, diag_inverse)


def solution(mesh):
    placed = (
        P("pole", None, None, "col", "row"),
        P("pole", None, ("row", "col"), None),
        P(),
        P("pole", None, "col", "row"),
        P("pole", None),
    )
    return jax.shard_map(
        body,
        mesh=mesh,
        in_specs=placed,
        out_specs=(P("pole", None, "row", "col"), P("pole", None, "col", "row"), P("col", "row")),
        check_vma=False,
    )
```

```python
import jax
import jax.numpy as jnp
from jax import lax
from jax.experimental import pallas as pl
from jax.experimental.pallas import tpu as pltpu
from jax.sharding import PartitionSpec as P

MESH = pl.DeviceIdType.MESH
F32 = jnp.float32
BF16 = jnp.bfloat16

E = 96
ROWS = 768
LN = 128
ORDER = (1, 2, 0, 3)


def copy_to(src, dst, send_sem, recv_sem, dev):
    return pltpu.make_async_remote_copy(
        src_ref=src,
        dst_ref=dst,
        send_sem=send_sem,
        recv_sem=recv_sem,
        device_id=dev,
        device_id_type=MESH,
    )


def dot(a, b, dims=(1, 0)):
    return lax.dot_general(
        a, b, (((dims[0],), (dims[1],)), ((), ())), preferred_element_type=F32
    )


def kernel(
    pat, wgt, g_hbm, p_hbm, d_hbm,
    x_out, id_out, den_out,
    g_in, p_in, d_in, gbuf, gt, lsrc, lbuf, loth, lrel, acc, xb, dsend, drecv, way, term, tpair, px, dh, dp,
    a_s, a_r, gz_s, gz_r, gy_s, gy_r, gr_s, gr_r, gc_s, gc_r,
    lp_s, lp_r, lm_s, lm_r, x_s, x_r, d_s, d_r, t_s, t_r, p_s, p_r, h_s, h_r, k_s, k_r, o_s, i_s,
):
    pole = lax.axis_index("pole")
    r = lax.axis_index("row")
    c = lax.axis_index("col")
    h = c // 4
    y = lax.rem(c, 4)
    z = 4 * h + r
    oth = 1 - h
    core = lax.rem(pole, 2)
    xx = pole // 2

    def at_y(d):
        return {"col": 4 * h + lax.rem(y + d, 4)}

    def at_z(d):
        zz = lax.rem(z + d, 8)
        return {"row": lax.rem(zz, 4), "col": (zz // 4) * 4 + y}

    def at_row(d):
        return {"row": lax.rem(r + d, 4)}

    def at_x(d):
        return {"pole": lax.rem(xx + d, 4) * 2 + core}

    partner = {"pole": 2 * xx + 1 - core}
    across = {"col": 4 * oth + y}

    loads = [
        pltpu.make_async_copy(src, dst, i_s.at[i])
        for i, (src, dst) in enumerate(((g_hbm, g_in), (p_hbm, p_in), (d_hbm, d_in)))
    ]
    for load in loads:
        load.start()

    bar = pltpu.get_barrier_semaphore()
    peers = [at_y(1), at_y(2), at_y(3), at_z(1), at_z(7), across, partner]
    peers += [at_row(d) for d in (1, 2, 3)] + [at_x(d) for d in (1, 2, 3)]
    for dev in peers:
        pl.semaphore_signal(bar, inc=1, device_id=dev, device_id_type=MESH)
    loads[0].wait()
    pl.semaphore_wait(bar, len(peers))

    def gz(t):
        return copy_to(g_in.at[0, t], gbuf.at[h, t, :, y], gz_s.at[t], gz_r.at[t], across)

    for t in (0, 1):
        gz(t).start()
    for load in loads[1:]:
        load.wait()

    @pl.when((r == 0) | (r == 3))
    def _():
        drecv[1] = jnp.zeros((2, 512, LN), BF16)

    fine = r * 8 + c
    for k in range(8):
        keep = pat[k, fine].astype(F32)
        for j in range(4):
            lo = k * 512 + ORDER[j] * LN
            for t in (0, 1):
                blk = p_in[0, t, :, lo:lo + LN].astype(F32) * keep
                lsrc[k, j, :, t * LN:(t + 1) * LN] = blk.astype(BF16)
    gbuf[h, :, :, y] = g_in[0]

    def to_col(d, which):
        k = (h if which == 0 else oth) * 4 + lax.rem(y + d, 4)
        dst = lbuf.at[:, z, y] if which == 0 else loth.at[:, y]
        return copy_to(lsrc.at[k], dst, a_s.at[d - 1, which], a_r.at[d - 1, which], at_y(d))

    for which in (1, 0):
        for d in (1, 3, 2):
            to_col(d, which).start()

    def gy(way, t):
        return copy_to(
            g_in.at[0, t], gbuf.at[h, t, :, y], gy_s.at[way, t], gy_r.at[way, t], at_y(1 if way == 0 else 3)
        )

    for i in (0, 1):
        gy(0, i).start()
        gy(1, 1 - i).start()

    lbuf[:, z, y] = lsrc[h * 4 + y]
    loth[:, y] = lsrc[oth * 4 + y]

    for which in (1, 0):
        for d in (1, 3, 2):
            to_col(d, which).wait_recv()

    def up(j, i, src, zp):
        return copy_to(src, lbuf.at[j, zp], lp_s.at[j, i], lp_r.at[j, i], at_z(1))

    def down(j, i, src, zp):
        return copy_to(src, lbuf.at[j, zp], lm_s.at[j, i], lm_r.at[j, i], at_z(7))

    def extra(j, d):
        return copy_to(loth.at[j], lrel.at[j], x_s.at[j], x_r.at[j], at_z(d))

    def launch_far(j):
        @pl.when(r == 2)
        def _():
            extra(j, 1).start()

        @pl.when(r == 1)
        def _():
            extra(j, 7).start()

        @pl.when(r == 3)
        def _():
            up(j, 0, loth.at[j], z).start()

        @pl.when(r == 0)
        def _():
            down(j, 0, loth.at[j], z).start()

    def launch(j):
        @pl.when(r < 3)
        def _():
            up(j, 0, lbuf.at[j, z], z).start()

        @pl.when(r > 0)
        def _():
            down(j, 0, lbuf.at[j, z], z).start()

    for j in range(4):
        launch_far(j)
    for j in (0, 1):
        launch(j)

    def relay(way):
        t = way
        frm = lax.rem(y + (3 if way == 0 else 1), 4)
        ref = gbuf.at[h, t, :, frm]
        return copy_to(ref, ref, gr_s.at[way], gr_r.at[way], at_y(1 if way == 0 else 3))

    gy(0, 0).wait_recv()
    relay(0).start()
    gy(1, 1).wait_recv()
    relay(1).start()

    def gc(d, t):
        ref = gbuf.at[oth, t, :, y]
        return copy_to(ref, ref, gc_s.at[d - 1, t], gc_r.at[d - 1, t], at_y(d))

    for t in (0, 1):
        gz(t).wait_recv()
        for d in (1, 3, 2):
            gc(d, t).start()

    gy(0, 1).wait_recv()
    gy(1, 0).wait_recv()
    relay(0).wait_recv()
    relay(1).wait_recv()

    def turn(half):
        @pl.loop(0, 4)
        def _(q):
            for t in (0, 1):
                gt[half * 4 + q, t] = gbuf[half, t, q].reshape(4 * E, ROWS).T

    turn(h)

    def compute(slot, j, zp):
        right = lbuf[j, zp].reshape(4 * E, 2 * LN)
        for t in (0, 1):
            acc[slot, t] += dot(gt[zp, t], right)

    def first(j):
        right = lbuf[j, z].reshape(4 * E, 2 * LN)
        for t in (0, 1):
            acc[j, t] = dot(gt[z, t], right)

    def edge(j):
        @pl.when(r == 3)
        def _():
            extra(j, 1).wait_recv()
            up(j, 1, lrel.at[j], 4 * h + 2).start()

        @pl.when(r == 0)
        def _():
            extra(j, 7).wait_recv()
            down(j, 1, lrel.at[j], 4 * h + 1).start()

    def relay_up(j, d, live=True):
        zp = lax.rem(z + 7 - d, 8)

        @pl.when((d < r + 2) & live)
        def _():
            up(j, d, lbuf.at[j, zp], zp).wait_recv()

            if d < 4:
                @pl.when(r < 3)
                def _():
                    up(j, d + 1, lbuf.at[j, zp], zp).start()

    def relay_down(j, d, live=True):
        zm = lax.rem(z + 1 + d, 8)

        @pl.when((d < 5 - r) & live)
        def _():
            down(j, d, lbuf.at[j, zm], zm).wait_recv()

            if d < 4:
                @pl.when(r > 0)
                def _():
                    down(j, d + 1, lbuf.at[j, zm], zm).start()

    def compute_up(j, d):
        @pl.when(d < r + 2)
        def _():
            compute(j, j, lax.rem(z + 7 - d, 8))

    def compute_down(j, d):
        @pl.when(d < 5 - r)
        def _():
            compute(j, j, lax.rem(z + 1 + d, 8))

    def compute_rest(j):
        @pl.loop(1, 8)
        def _(k):
            compute(j, j, lax.rem(z + k, 8))

    def out_copy(j):
        cols = pl.ds(ORDER[j] * LN, LN)
        return [
            pltpu.make_async_copy(
                xb.at[j, :, pl.ds(t * LN, LN)], x_out.at[0, t, :, cols], o_s.at[j, t]
            )
            for t in (0, 1)
        ]

    def finish(slot, j):
        @pl.loop(0, 8)
        def _(b):
            rows = pl.ds(b * E, E)
            re = acc[slot, 1, rows, LN:] - acc[slot, 0, rows, :LN]
            im = -(acc[slot, 0, rows, LN:] + acc[slot, 1, rows, :LN])
            xb[j, rows, :LN] = re.astype(BF16)
            xb[j, rows, LN:] = im.astype(BF16)

        for one in out_copy(j):
            one.start()

    def diag(jb, start=0, stop=4):
        @pl.loop(start, stop)
        def _(ja):
            low = lbuf[ja, r].reshape(4 * E, 2 * LN)
            high = lbuf[ja, 4 + r].reshape(4 * E, 2 * LN)
            both = dot(low, xb[jb, :4 * E], (0, 0)) + dot(high, xb[jb, 4 * E:], (0, 0))
            rows = pl.ds(pl.multiple_of(ja * LN, LN), LN)
            dsend[ORDER[jb], 0, rows, :] = (both[:LN, :LN] - both[LN:, LN:]).astype(BF16)
            dsend[ORDER[jb], 1, rows, :] = (both[:LN, LN:] + both[LN:, :LN]).astype(BF16)

    for d in range(5):
        for j in (0, 1):
            if d == 0:
                edge(j)
            relay_up(j, d)
            relay_down(j, d)
        if d == 2:
            for j in (2, 3):
                launch(j)
                edge(j)
            for i in (0, 1):
                for j in (2, 3):
                    relay_up(j, i, r == 0)
                    relay_down(j, i, r == 3)
    def share(j, part):
        own = ORDER[j]
        d = lax.rem(own + 4 - r, 4) - 1
        slot = jnp.maximum(d, 0)
        rows = pl.ds(part * 2 * LN, 2 * LN)
        return copy_to(
            dsend.at[own, :, rows], drecv.at[slot, :, rows], d_s.at[slot, part], d_r.at[slot, part], {"row": own}
        )

    def give(j, part):
        @pl.when(r != ORDER[j])
        def _():
            share(j, part).start()

    def give_both(j):
        share(j, 0).start()
        share(j, 1).start()

    for d in range(5):
        relay_up(2, d, r > 0)
        relay_down(3, d, r < 3)
        if d > 0:
            relay_up(3, d - 1, r > 0)
            relay_down(2, d - 1, r < 3)
        if d == 0:
            continue
        if d == 1:
            for t in (0, 1):
                for i in (1, 3, 2):
                    gc(i, t).wait_recv()
            turn(oth)
            first(2)
            first(3)
            compute_up(2, 0)
            compute_down(3, 0)
        compute_up(2, d)
        compute_down(3, d)
        compute_up(3, d - 1)
        compute_down(2, d - 1)
        if d < 3:
            first(d - 1)
            compute_rest(d - 1)
            finish(d - 1, d - 1)
        if d == 2:
            diag(0, 0, 2)
            diag(1, 0, 2)
            give(0, 0)
            give(1, 0)
        if d == 4:
            diag(0, 2, 4)
            diag(1, 2, 4)
            give(0, 1)
            give(1, 1)

    @pl.when(r > 0)
    def _():
        finish(2, 2)
        diag(2)

    @pl.when(r < 3)
    def _():
        finish(3, 3)
        diag(3)

    def meet(own):
        return copy_to(dsend.at[own], way, k_s, k_r, {"row": 3 - r})

    def pass_on(own, j):
        meet(3 - own).start()
        meet(own).wait_recv()
        for t in (0, 1):
            dsend[own, t] = (dsend[own, t].astype(F32) + way[t].astype(F32)).astype(BF16)
        give_both(j)

    @pl.when(r == 1)
    def _():
        pass_on(0, 2)

    @pl.when(r == 2)
    def _():
        pass_on(3, 3)

    @pl.when(r == 3)
    def _():
        give_both(2)
        relay_up(3, 4)
        compute_up(3, 4)
        finish(3, 3)
        diag(3)

    @pl.when(r == 0)
    def _():
        give_both(3)
        relay_down(2, 4)
        compute_down(2, 4)
        finish(2, 2)
        diag(2)

    def got(d, part):
        rows = pl.ds(part * 2 * LN, 2 * LN)
        return copy_to(
            dsend.at[r, :, rows], drecv.at[d, :, rows], d_s.at[d, part], d_r.at[d, part], partner
        )

    for part in (0, 1):
        got(0, part).wait_recv()
        got(2, part).wait_recv()

        @pl.when((r == 1) | (r == 2))
        def _():
            got(1, part).wait_recv()

    for j in range(4):
        rows = pl.ds(j * LN, LN)
        cols = pl.ds(ORDER[j] * LN, LN)
        part = []
        for t in (0, 1):
            sum_ = dsend[r, t, rows, :].astype(F32)
            for d in range(3):
                sum_ += drecv[d, t, rows, :].astype(F32)
            part.append(d_in[0, t, cols, :].astype(F32) - sum_)
            id_out[0, t, cols, :] = part[t].astype(BF16)
        term[cols, :] = wgt[0, 0] * part[1] + wgt[0, 1] * part[0]

    mine = pl.ds(pl.multiple_of(core * 256, 256), 256)
    other = pl.ds(pl.multiple_of((1 - core) * 256, 256), 256)
    pair = copy_to(term.at[other], tpair, t_s, t_r, partner)
    pair.start()
    pair.wait_recv()
    px[xx] = (term[mine, :] + tpair[...]).astype(BF16)

    def along(d):
        return copy_to(px.at[xx], px.at[xx], p_s.at[d - 1], p_r.at[d - 1], at_x(d))

    for d in (1, 3, 2):
        along(d).start()
    for d in (1, 3, 2):
        along(d).wait_recv()
    half = px[0].astype(F32)
    for k in range(1, 4):
        half += px[k].astype(F32)
    dh[...] = half
    den_out[mine, :] = half
    swap = copy_to(dh, dp, h_s, h_r, partner)
    swap.start()
    swap.wait_recv()
    den_out[other, :] = dp[...]

    for t in (0, 1):
        gz(t).wait_send()
        gy(0, t).wait_send()
        gy(1, t).wait_send()
        relay(t).wait_send()
        for d in (1, 2, 3):
            gc(d, t).wait_send()
            to_col(d, t).wait_send()
    for j in (0, 1):
        @pl.when(r != ORDER[j])
        def _():
            for part in (0, 1):
                share(j, part).wait_send()

    for part in (0, 1):
        @pl.when((r == 1) | (r == 3))
        def _():
            share(2, part).wait_send()

        @pl.when((r == 0) | (r == 2))
        def _():
            share(3, part).wait_send()

    @pl.when((r == 1) | (r == 2))
    def _():
        meet(0).wait_send()

    for d in (1, 2, 3):
        along(d).wait_send()
    pair.wait_send()
    swap.wait_send()

    @pl.loop(0, 4)
    def _(j):
        @pl.when((r == 1) | (r == 2))
        def _():
            extra(j, 1).wait_send()

        @pl.loop(0, 5)
        def _(i):
            @pl.when(((r < 3) & (i < r + 3)) | ((r == 3) & (i < 2)))
            def _():
                up(j, i, lbuf.at[j, z], z).wait_send()

            @pl.when(((r > 0) & (i < 6 - r)) | ((r == 0) & (i < 2)))
            def _():
                down(j, i, lbuf.at[j, z], z).wait_send()

    for j in range(4):
        for one in out_copy(j):
            one.wait()


def body(anc_inverse, panel, pattern, diag_inverse, pole_weights):
    vmem = pl.BlockSpec(memory_space=pltpu.VMEM)
    hbm = pl.BlockSpec(memory_space=pl.ANY)
    smem = pl.BlockSpec(memory_space=pltpu.SMEM)
    dma = pltpu.SemaphoreType.DMA
    sems = [(3, 2), (2,), (2, 2), (2,), (3, 2), (4, 5), (4, 5), (4,), (3, 2), None, (3,), None, None]
    pairs = []
    for shape in sems:
        one = dma if shape is None else dma(shape)
        pairs += [one, one]
    inv_panel, inv_diag, density = pl.pallas_call(
        kernel,
        out_shape=(
            jax.ShapeDtypeStruct((1, 2, ROWS, 512), BF16),
            jax.ShapeDtypeStruct((1, 2, 512, LN), BF16),
            jax.ShapeDtypeStruct((512, LN), F32),
        ),
        in_specs=[smem, smem, hbm, hbm, hbm],
        out_specs=(hbm, vmem, vmem),
        scratch_shapes=[
            pltpu.VMEM((1, 2, 4, E, ROWS), BF16),
            pltpu.VMEM((1, 2, E, 4096), BF16),
            pltpu.VMEM((1, 2, 512, LN), BF16),
            pltpu.VMEM((2, 2, 4, 4, E, ROWS), BF16),
            pltpu.VMEM((8, 2, ROWS, 4 * E), BF16),
            pltpu.VMEM((8, 4, E, 2 * LN), BF16),
            pltpu.VMEM((4, 8, 4, E, 2 * LN), BF16),
            pltpu.VMEM((4, 4, E, 2 * LN), BF16),
            pltpu.VMEM((4, 4, E, 2 * LN), BF16),
            pltpu.VMEM((4, 2, ROWS, 2 * LN), F32),
            pltpu.VMEM((4, ROWS, 2 * LN), BF16),
            pltpu.VMEM((4, 2, 512, LN), BF16),
            pltpu.VMEM((3, 2, 512, LN), BF16),
            pltpu.VMEM((2, 512, LN), BF16),
            pltpu.VMEM((512, LN), F32),
            pltpu.VMEM((256, LN), F32),
            pltpu.VMEM((4, 256, LN), BF16),
            pltpu.VMEM((256, LN), F32),
            pltpu.VMEM((256, LN), F32),
            *pairs,
            dma((4, 2)),
            dma((3,)),
        ],
        compiler_params=pltpu.CompilerParams(
            collective_id=0, has_side_effects=True, vmem_limit_bytes=60 * 1024 * 1024
        ),
    )(pattern.T, pole_weights, anc_inverse, panel, diag_inverse)
    return inv_panel.astype(F32), inv_diag, density


def solution(mesh):
    placed = (
        P("pole", None, None, "col", "row"),
        P("pole", None, ("row", "col"), None),
        P(),
        P("pole", None, "col", "row"),
        P("pole", None),
    )
    return jax.shard_map(
        body,
        mesh=mesh,
        in_specs=placed,
        out_specs=(P("pole", None, "row", "col"), P("pole", None, "col", "row"), P("col", "row")),
        check_vma=False,
    )
```
